32 devices in a mesh: gx: 4 (over y, core), gy: 8 (over z, x).
Axes of the slice: x: 2, y: 2, z: 4, core: 2. Of those that a mesh axis runs over, the one named last changes fastest.
Arguments:
- pixels: int32 [16, 16, 4, 131072], P('gy', 'gx'), may hold values from 0 to 255, as said below
- weights: bfloat16 [16, 16, 4, 131072], P('gy', 'gx'), may hold values from 0.25 to 1
- adjacency: int32 [2, 16, 16], replicated, may hold values 0 or 1
Outputs:
- log_gain: float32 [16, 16], P('gy', 'gx')
The draws below stay inside these ranges and needn't reach their ends.
Inputs may be any that keep to these rules, and one draw needn't show every extreme that they name: `pixels`: bin indices of 8-bit intensities. `adjacency`: entry [0, r, c] is 1 where tile (r, c) and the tile to its right share a usable border, entry [1, r, c] likewise for the tile below; entries of pairs beyond the grid's edge are read by no output.
All inputs are finite; a program needn't handle non-finite values.
Results may differ from the reference program's by a relative error of at most 0.0003.
Values may be sent and summed in bfloat16 or wider, within the bound.
A program may use at most 128 MiB of HBM per device.

```python
import math
import jax
import jax.numpy as jnp
from jax import lax

SEG = 1024
STRIP = 128
ITERS = 20
GR = 16
GC = 16


def draw_pixels(key, part):
    offset_key = jax.random.fold_in(key, 11)
    spread_key = jax.random.fold_in(key, 12)
    jitter_key = jax.random.fold_in(key, 13)
    slope_key = jax.random.fold_in(key, 14)
    length = STRIP * SEG
    column = jnp.arange(GC, dtype=jnp.int32)
    drift = 32 * column // GC
    baseline = drift[None, :] + jax.random.randint(offset_key, (GR, GC), 0, 32, dtype=jnp.int32)
    slope = jax.random.randint(slope_key, (GR, GC, 4, 1), -80, 81, dtype=jnp.int32)
    position = jnp.arange(length, dtype=jnp.int32)[None, None, None, :]
    ramp = 80 + slope * position // length
    spread = jax.random.randint(spread_key, (GR, GC, 4), 20, 61, dtype=jnp.int32)
    jitter = jax.random.randint(jitter_key, (GR, GC, 4, length), 0, spread[..., None], dtype=jnp.int32)
    return jnp.clip(baseline[:, :, None, None] + ramp + jitter, 0, 255).astype(jnp.int32)


def draw_weights(key, part):
    phase_key = jax.random.fold_in(key, 21)
    rough_key = jax.random.fold_in(key, 22)
    length = STRIP * SEG
    along = jnp.arange(length, dtype=jnp.float32) / length
    phase = jax.random.uniform(phase_key, (GR, GC, 4, 1), jnp.float32, -math.pi, math.pi)
    wave = 0.5 + 0.5 * jnp.sin(math.pi * along[None, None, None, :] + phase)
    rough = jax.random.uniform(rough_key, (GR, GC, 4, length), jnp.float32, 0.7, 1.0)
    profile = wave
    return (0.25 + 0.75 * rough * profile).astype(jnp.bfloat16)


def set_ends(array, key, smallest, top_value):
    spot = [jax.random.randint(jax.random.fold_in(key, axis), (), 0, length) for axis, length in enumerate(array.shape)]
    widest = array.shape.index(max(array.shape))
    neighbour = spot[:widest] + [(spot[widest] + 1) % array.shape[widest]] + spot[widest + 1:]
    return array.at[tuple(spot)].set(smallest).at[tuple(neighbour)].set(top_value)


def setup_inputs(seed: int = 0) -> dict:
    arg_keys = jax.random.split(jax.random.key(seed), 4)
    pixels = draw_pixels(jax.random.fold_in(arg_keys[3], 71), 0)
    weights = draw_weights(jax.random.fold_in(arg_keys[3], 71), 0)
    adjacency = set_ends((jax.random.randint(arg_keys[2], (2, GR, GC), 0, 8) < 7).astype(jnp.int32), jax.random.fold_in(arg_keys[2], 1), 0, 1)
    return dict(pixels=pixels, weights=weights, adjacency=adjacency)


anchor_weight = 0.5
mismatch_scale = 8.0


def strip_stats(strip_hist):
    totals = jnp.sum(strip_hist, axis=-1)
    centres = jnp.arange(256, dtype=jnp.float32) + 0.5
    means = jnp.sum(strip_hist * centres, axis=-1) / totals
    cumulative = jnp.cumsum(strip_hist, axis=-1) / totals[..., None]
    return means, cumulative


def pair_terms(own_hist, other_hist, usable):
    own_mean, own_cdf = strip_stats(own_hist)
    other_mean, other_cdf = strip_stats(other_hist)
    distance = jnp.sum(jnp.abs(own_cdf - other_cdf), axis=-1)
    mismatch = (distance - jnp.abs(own_mean - other_mean)) / mismatch_scale
    present = usable > 0
    confidence = jnp.where(present, 1.0 / (0.25 + mismatch * mismatch), 0.0)
    offsets = jnp.where(present, jnp.log(other_mean) - jnp.log(own_mean), 0.0)
    return confidence, offsets


def relax_step(padded, confidence, offsets):
    beside = jnp.stack([padded[:-2, 1:-1], padded[2:, 1:-1], padded[1:-1, :-2], padded[1:-1, 2:]], axis=-1)
    return jnp.sum(confidence * (beside + offsets), axis=-1)


def reference(pixels, weights, adjacency):
    length = pixels.shape[3]

    def row_histogram(row_index):
        own_pixels = lax.dynamic_index_in_dim(pixels, row_index, 0, False)
        own_weights = lax.dynamic_index_in_dim(weights, row_index, 0, False).astype(jnp.float32)
        below_index = jnp.minimum(row_index + 1, GR - 1).astype(jnp.int32)
        above_index = jnp.maximum(row_index - 1, 0).astype(jnp.int32)
        from_below = lax.dynamic_index_in_dim(weights, below_index, 0, False)[:, 0].astype(jnp.float32)
        from_below = from_below * (row_index + 1 < GR).astype(jnp.float32)
        from_above = lax.dynamic_index_in_dim(weights, above_index, 0, False)[:, 1].astype(jnp.float32)
        from_above = from_above * (row_index > 0).astype(jnp.float32)
        zero_strip = jnp.zeros((1, length), jnp.float32)
        from_left = jnp.concatenate([zero_strip, own_weights[:-1, 3]], axis=0)
        from_right = jnp.concatenate([own_weights[1:, 2], zero_strip], axis=0)
        partner = jnp.stack([from_above, from_below, from_left, from_right], axis=1)
        joint_weight = lax.optimization_barrier((own_weights * partner).astype(jnp.bfloat16)).astype(jnp.float32)
        strip_ids = (jnp.arange(GC * 4, dtype=jnp.int32) * 256)[:, None]
        segment = (strip_ids + own_pixels.reshape(GC * 4, length).astype(jnp.int32)).reshape(-1)
        bin_sums = jax.ops.segment_sum(joint_weight.reshape(-1), segment, num_segments=GC * 4 * 256)
        return bin_sums.reshape(GC, 4, 256)

    strip_hist = lax.map(row_histogram, jnp.arange(GR, dtype=jnp.int32))
    zero_row = jnp.zeros((1, GC, 256), jnp.float32)
    zero_column = jnp.zeros((GR, 1, 256), jnp.float32)
    from_above = jnp.concatenate([zero_row, strip_hist[:-1, :, 1]], axis=0)
    from_below = jnp.concatenate([strip_hist[1:, :, 0], zero_row], axis=0)
    from_left = jnp.concatenate([zero_column, strip_hist[:, :-1, 3]], axis=1)
    from_right = jnp.concatenate([strip_hist[:, 1:, 2], zero_column], axis=1)
    partner_hist = jnp.stack([from_above, from_below, from_left, from_right], axis=2)
    across = adjacency[0].astype(jnp.int32)
    downward = adjacency[1].astype(jnp.int32)
    zero_links_row = jnp.zeros((1, GC), jnp.int32)
    zero_links_column = jnp.zeros((GR, 1), jnp.int32)
    up_valid = jnp.concatenate([zero_links_row, downward[:-1]], axis=0)
    down_valid = jnp.concatenate([downward[:-1], zero_links_row], axis=0)
    left_valid = jnp.concatenate([zero_links_column, across[:, :-1]], axis=1)
    right_valid = jnp.concatenate([across[:, :-1], zero_links_column], axis=1)
    usable = jnp.stack([up_valid, down_valid, left_valid, right_valid], axis=-1)
    confidence, offsets = pair_terms(strip_hist, partner_hist, usable)
    denominator = anchor_weight + jnp.sum(confidence, axis=-1)
    log_gain = jnp.zeros((GR, GC), jnp.float32)
    for sweep_index in range(ITERS):
        updated = relax_step(jnp.pad(log_gain, 1), confidence, offsets) / denominator
        log_gain = updated - jnp.sum(updated) / (GR * GC)
    return log_gain
```

```python
import functools
import jax
import jax.numpy as jnp
from jax import lax
from jax.experimental import pallas as pl
from jax.experimental.pallas import tpu as pltpu
from jax.sharding import PartitionSpec as P

ITERS = 20
WIDTH = 4096
SUBS = 4
PER_DOT = 4


anchor_weight = 0.5
mismatch_scale = 8.0


def chunk_width(length):
    width = WIDTH
    while length % width:
        width //= 2
    return width


def one_hots(bins, joint, level, shape):
    bins16 = jnp.broadcast_to(bins, shape).astype(jnp.int16)
    upper = (bins16 & 240) == level * 16
    lower = (bins16 & 15) == level
    joint16 = jnp.broadcast_to(joint, shape).astype(jnp.bfloat16)
    zero = jnp.zeros(shape, jnp.bfloat16)
    return jnp.where(upper, joint16, zero), jnp.where(lower, jnp.ones(shape, jnp.bfloat16), zero)


def accumulate(dots, read_bins, read_joint, sums, width):
    depth = width // SUBS
    shape = (16, depth)
    level = lax.broadcasted_iota(jnp.int32, shape, 0).astype(jnp.int16)
    for index, strips in enumerate(dots):
        left, right = [], []
        for strip in strips:
            for sub in range(SUBS):
                lanes = slice(sub * depth, (sub + 1) * depth)
                first, second = one_hots(read_bins(strip, lanes), read_joint(strip, lanes), level, shape)
                left.append(first)
                right.append(second)
        left = jnp.concatenate(left, axis=0)
        right = jnp.concatenate(right, axis=0)
        counts = lax.dot_general(
            left, right, (((1,), (1,)), ((), ())), preferred_element_type=jnp.float32
        )
        sums[index] += counts


def finish(dots, sums, out_ref):
    place = 0
    for index, strips in enumerate(dots):
        for number in range(len(strips)):
            total = jnp.zeros((16, 16), jnp.float32)
            for sub in range(SUBS):
                start = (number * SUBS + sub) * 16
                total += sums[index, start : start + 16, start : start + 16]
            out_ref[place] = total
            place += 1


def group(strips):
    return [strips[i : i + PER_DOT] for i in range(0, len(strips), PER_DOT)]


def inner_strips(rows, columns):
    strips = []
    for row in range(rows - 1):
        for column in range(columns):
            strips += [(row, column, 1), (row + 1, column, 0)]
    for row in range(rows):
        for column in range(columns - 1):
            strips += [(row, column, 3), (row, column + 1, 2)]
    return strips


def outer_strips(rows, columns):
    strips = [(0, column, 0) for column in range(columns)]
    strips += [(rows - 1, column, 1) for column in range(columns)]
    strips += [(row, 0, 2) for row in range(rows)]
    strips += [(row, columns - 1, 3) for row in range(rows)]
    return strips


def partner_of(strip):
    row, column, side = strip
    return [
        (row - 1, column, 1),
        (row + 1, column, 0),
        (row, column - 1, 3),
        (row, column + 1, 2),
    ][side]


def edges_kernel(w_ref, up_ref, down_ref, left_ref, right_ref):
    rows, columns = w_ref.shape[:2]
    for column in range(columns):
        up_ref[column : column + 1] = w_ref[0, column, 0:1, :]
        down_ref[column : column + 1] = w_ref[rows - 1, column, 1:2, :]
    for row in range(rows):
        left_ref[row : row + 1] = w_ref[row, 0, 2:3, :]
        right_ref[row : row + 1] = w_ref[row, columns - 1, 3:4, :]


def edges(weights):
    rows, columns, sides, length = weights.shape
    width = chunk_width(length)
    row_shape = jax.ShapeDtypeStruct((columns, length), weights.dtype)
    column_shape = jax.ShapeDtypeStruct((rows, length), weights.dtype)
    row_spec = pl.BlockSpec((columns, width), lambda i: (0, i))
    column_spec = pl.BlockSpec((rows, width), lambda i: (0, i))
    return pl.pallas_call(
        edges_kernel,
        grid=(length // width,),
        in_specs=[pl.BlockSpec((rows, columns, sides, width), lambda i: (0, 0, 0, i))],
        out_specs=[row_spec, row_spec, column_spec, column_spec],
        out_shape=[row_shape, row_shape, column_shape, column_shape],
        name="edges",
    )(weights)


def inner_kernel(dots, p_ref, w_ref, out_ref, wide, sums):
    @pl.when(pl.program_id(0) == 0)
    def _():
        sums[...] = jnp.zeros_like(sums)

    wide[...] = w_ref[...].astype(jnp.float32)

    def read_bins(strip, lanes):
        row, column, side = strip
        return p_ref[row, column, side : side + 1, lanes]

    def read_joint(strip, lanes):
        row, column, side = strip
        if side in (0, 2):
            row, column, side = partner_of(strip)
        other_row, other_column, other_side = partner_of((row, column, side))
        return (
            wide[row, column, side : side + 1, lanes]
            * wide[other_row, other_column, other_side : other_side + 1, lanes]
        )

    accumulate(dots, read_bins, read_joint, sums, p_ref.shape[-1])

    @pl.when(pl.program_id(0) == pl.num_programs(0) - 1)
    def _():
        finish(dots, sums, out_ref)


def outer_kernel(dots, p_ref, w_ref, up_ref, down_ref, left_ref, right_ref, out_ref, wide, row_wide, column_wide, sums):
    @pl.when(pl.program_id(0) == 0)
    def _():
        sums[...] = jnp.zeros_like(sums)

    wide[...] = w_ref[...].astype(jnp.float32)
    row_wide[0] = up_ref[...].astype(jnp.float32)
    row_wide[1] = down_ref[...].astype(jnp.float32)
    column_wide[0] = left_ref[...].astype(jnp.float32)
    column_wide[1] = right_ref[...].astype(jnp.float32)

    def read_bins(strip, lanes):
        row, column, side = strip
        return p_ref[row, column, side : side + 1, lanes]

    def read_joint(strip, lanes):
        row, column, side = strip
        own = wide[row, column, side : side + 1, lanes]
        if side < 2:
            return own * row_wide[side, column : column + 1, lanes]
        return own * column_wide[side - 2, row : row + 1, lanes]

    accumulate(dots, read_bins, read_joint, sums, p_ref.shape[-1])

    @pl.when(pl.program_id(0) == pl.num_programs(0) - 1)
    def _():
        finish(dots, sums, out_ref)


def strip_sums(kernel, strips, pixels, weights, halos, name):
    rows, columns, sides, length = pixels.shape
    width = chunk_width(length)
    dots = group(strips)
    block = (rows, columns, sides, width)
    halo_specs = [pl.BlockSpec((h.shape[0], width), lambda i: (0, i)) for h in halos]
    scratch = [pltpu.VMEM(block, jnp.float32)]
    if halos:
        scratch += [pltpu.VMEM((2, columns, width), jnp.float32), pltpu.VMEM((2, rows, width), jnp.float32)]
    scratch += [pltpu.VMEM((len(dots), 16 * SUBS * PER_DOT, 16 * SUBS * PER_DOT), jnp.float32)]
    return pl.pallas_call(
        functools.partial(kernel, dots),
        grid=(length // width,),
        in_specs=[pl.BlockSpec(block, lambda i: (0, 0, 0, i))] * 2 + halo_specs,
        out_specs=pl.BlockSpec((len(strips), 16, 16), lambda i: (0, 0, 0)),
        out_shape=jax.ShapeDtypeStruct((len(strips), 16, 16), jnp.float32),
        scratch_shapes=scratch,
        compiler_params=pltpu.CompilerParams(vmem_limit_bytes=56 * 1024 * 1024),
        cost_estimate=pl.CostEstimate(
            flops=len(strips) * length * 256 * 32,
            bytes_accessed=rows * columns * sides * length * 6,
            transcendentals=0,
        ),
        name=name,
    )(pixels, weights, *halos)


def shift(array, axis, step):
    count = lax.axis_size(axis)
    if step > 0:
        pairs = [(i, i + 1) for i in range(count - 1)]
    else:
        pairs = [(i + 1, i) for i in range(count - 1)]
    return lax.ppermute(array, axis, pairs)


def histograms(pixels, weights):
    rows, columns, sides, length = pixels.shape
    up, down, left, right = edges(weights)
    from_up = shift(down, "gy", 1)
    from_down = shift(up, "gy", -1)
    from_left = shift(right, "gx", 1)
    from_right = shift(left, "gx", -1)
    inner = inner_strips(rows, columns)
    outer = outer_strips(rows, columns)
    inner_sums = strip_sums(inner_kernel, inner, pixels, weights, [], "inner")
    outer_sums = strip_sums(
        outer_kernel, outer, pixels, weights, [from_up, from_down, from_left, from_right], "outer"
    )
    sums = jnp.concatenate([inner_sums, outer_sums], axis=0).reshape(-1, 256)
    place = {strip: i for i, strip in enumerate(inner + outer)}
    order = [place[(r, c, s)] for r in range(rows) for c in range(columns) for s in range(sides)]
    return jnp.stack([sums[i] for i in order]).reshape(rows, columns, sides, 256)


def padded_2(block, sides, width):
    for axis, dim in sides:
        count = lax.axis_size(axis)
        forward = [(i, i + 1) for i in range(count - 1)]
        backward = [(target, source) for source, target in forward]
        low = lax.ppermute(
            lax.slice_in_dim(block, block.shape[dim] - width, None, axis=dim), axis, forward
        )
        high = lax.ppermute(lax.slice_in_dim(block, 0, width, axis=dim), axis, backward)
        block = jnp.concatenate([low, block, high], axis=dim)
    return block


def column_edges(source):
    return jnp.stack([source[:, 0, 2], source[:, -1, 3]], axis=1)


def row_edges(source):
    return jnp.stack([source[0, :, 0], source[-1, :, 1]], axis=0)


def facing(source, column_halo, row_halo):
    side_right = jnp.concatenate([source[:, 1:, 2], column_halo[:, 3:4]], axis=1)
    side_left = jnp.concatenate([column_halo[:, 0:1], source[:, :-1, 3]], axis=1)
    side_down = jnp.concatenate([source[1:, :, 0], row_halo[3:4]], axis=0)
    side_up = jnp.concatenate([row_halo[0:1], source[:-1, :, 1]], axis=0)
    return jnp.stack([side_up, side_down, side_left, side_right], axis=2)


def strip_stats(strip_hist):
    indices = jnp.arange(256, dtype=jnp.int32)
    triangle = (indices[:, None] <= indices[None, :]).astype(jnp.float32)
    totals = jnp.sum(strip_hist, axis=-1)
    centres = indices.astype(jnp.float32) + 0.5
    means = jnp.sum(strip_hist * centres, axis=-1) / totals
    cumulative = jnp.dot(strip_hist, triangle, precision=lax.Precision.HIGHEST) / totals[..., None]
    return (means, cumulative)


def pair_terms(own_hist, other_hist, usable):
    own_mean, own_cdf = strip_stats(own_hist)
    other_mean, other_cdf = strip_stats(other_hist)
    distance = jnp.sum(jnp.abs(own_cdf - other_cdf), axis=-1)
    mismatch = (distance - jnp.abs(own_mean - other_mean)) / mismatch_scale
    present = usable > 0
    confidence = jnp.where(present, 1.0 / (0.25 + mismatch * mismatch), 0.0)
    offsets = jnp.where(present, jnp.log(other_mean) - jnp.log(own_mean), 0.0)
    return (confidence, offsets)


def relax_step(padded, confidence, offsets):
    beside = jnp.stack(
        [padded[:-2, 1:-1], padded[2:, 1:-1], padded[1:-1, :-2], padded[1:-1, 2:]], axis=-1
    )
    return jnp.sum(confidence * (beside + offsets), axis=-1)


def body(pixels, weights, adjacency):
    tile_rows, tile_columns = (pixels.shape[0], pixels.shape[1])
    grid_rows = tile_rows * lax.axis_size("gy")
    grid_columns = tile_columns * lax.axis_size("gx")
    row_start = lax.axis_index("gy") * tile_rows
    column_start = lax.axis_index("gx") * tile_columns
    tile_count = grid_rows * grid_columns
    strip_hist = histograms(pixels, weights)
    column_hist = padded_2(column_edges(strip_hist), (("gx", 1),), 1)
    row_hist = padded_2(row_edges(strip_hist), (("gy", 0),), 1)
    partner_hist = facing(strip_hist, column_hist, row_hist)
    padded_links = jnp.pad(adjacency, ((0, 0), (1, 1), (1, 1)))
    block_shape = (tile_rows, tile_columns)
    global_row = row_start + jnp.arange(tile_rows, dtype=jnp.int32)[:, None]
    global_column = column_start + jnp.arange(tile_columns, dtype=jnp.int32)[None, :]
    up_valid = lax.dynamic_slice(padded_links[1], (row_start, column_start + 1), block_shape)
    down_valid = lax.dynamic_slice(padded_links[1], (row_start + 1, column_start + 1), block_shape)
    down_valid = down_valid * (global_row < grid_rows - 1).astype(jnp.int32)
    left_valid = lax.dynamic_slice(padded_links[0], (row_start + 1, column_start), block_shape)
    right_valid = lax.dynamic_slice(padded_links[0], (row_start + 1, column_start + 1), block_shape)
    right_valid = right_valid * (global_column < grid_columns - 1).astype(jnp.int32)
    usable = jnp.stack([up_valid, down_valid, left_valid, right_valid], axis=-1)
    confidence, offsets = pair_terms(strip_hist, partner_hist, usable)
    pair_rows = jnp.stack(
        [confidence[..., 1], offsets[..., 1], confidence[..., 3], offsets[..., 3]], axis=0
    )
    gathered = lax.all_gather(pair_rows[None], ("gx", "gy"), axis=0, tiled=True)
    width_x = lax.axis_size("gx")
    width_y = lax.axis_size("gy")
    full_grid = gathered.reshape(width_x, width_y, 4, tile_rows, tile_columns)
    full_grid = full_grid.transpose(2, 1, 3, 0, 4).reshape(4, grid_rows, grid_columns)
    down_conf, down_offset = (full_grid[0], full_grid[1])
    right_conf, right_offset = (full_grid[2], full_grid[3])
    up_conf = jnp.pad(down_conf[:-1], ((1, 0), (0, 0)))
    up_offset = -jnp.pad(down_offset[:-1], ((1, 0), (0, 0)))
    left_conf = jnp.pad(right_conf[:, :-1], ((0, 0), (1, 0)))
    left_offset = -jnp.pad(right_offset[:, :-1], ((0, 0), (1, 0)))
    global_conf = jnp.stack([up_conf, down_conf, left_conf, right_conf], axis=-1)
    global_offset = jnp.stack([up_offset, down_offset, left_offset, right_offset], axis=-1)
    global_denominator = anchor_weight + jnp.sum(global_conf, axis=-1)

    def global_sweep(sweep_index, log_gain):
        updated = relax_step(jnp.pad(log_gain, 1), global_conf, global_offset) / global_denominator
        return updated - jnp.sum(updated) / tile_count

    whole_gain = lax.fori_loop(
        0, ITERS, global_sweep, jnp.zeros((grid_rows, grid_columns), jnp.float32)
    )
    return lax.dynamic_slice(whole_gain, (row_start, column_start), block_shape)


def solution(mesh):
    return jax.shard_map(
        body,
        mesh=mesh,
        in_specs=(P("gy", "gx", None, None), P("gy", "gx", None, None), P()),
        out_specs=P("gy", "gx"),
        check_vma=False,
    )
```

```python
import functools
import jax
import jax.numpy as jnp
from jax import lax
from jax.experimental import pallas as pl
from jax.experimental.pallas import tpu as pltpu
from jax.sharding import PartitionSpec as P

ITERS = 20
WIDTH = 4096
SUBS = 4
PER_DOT = 4


anchor_weight = 0.5
mismatch_scale = 8.0


def chunk_width(length):
    width = WIDTH
    while length % width:
        width //= 2
    return width


def one_hots(bins, joint, level, shape):
    bins16 = jnp.broadcast_to(bins, shape).astype(jnp.int16)
    upper = (bins16 & 240) == level * 16
    lower = (bins16 & 15) == level
    joint16 = jnp.broadcast_to(joint, shape).astype(jnp.bfloat16)
    zero = jnp.zeros(shape, jnp.bfloat16)
    return jnp.where(upper, joint16, zero), jnp.where(lower, jnp.ones(shape, jnp.bfloat16), zero)


def accumulate(dots, read_bins, read_joint, sums, width):
    depth = width // SUBS
    shape = (16, depth)
    level = lax.broadcasted_iota(jnp.int32, shape, 0).astype(jnp.int16)
    for index, strips in enumerate(dots):
        left, right = [], []
        for strip in strips:
            for sub in range(SUBS):
                lanes = slice(sub * depth, (sub + 1) * depth)
                first, second = one_hots(read_bins(strip, lanes), read_joint(strip, lanes), level, shape)
                left.append(first)
                right.append(second)
        left = jnp.concatenate(left, axis=0)
        right = jnp.concatenate(right, axis=0)
        counts = lax.dot_general(
            left, right, (((1,), (1,)), ((), ())), preferred_element_type=jnp.float32
        )
        sums[index] += counts


def finish(dots, sums, out_ref):
    place = 0
    for index, strips in enumerate(dots):
        for number in range(len(strips)):
            total = jnp.zeros((16, 16), jnp.float32)
            for sub in range(SUBS):
                start = (number * SUBS + sub) * 16
                total += sums[index, start : start + 16, start : start + 16]
            out_ref[place] = total
            place += 1


def group(strips):
    return [strips[i : i + PER_DOT] for i in range(0, len(strips), PER_DOT)]


def inner_strips(rows, columns):
    strips = []
    for row in range(rows - 1):
        for column in range(columns):
            strips += [(row, column, 1), (row + 1, column, 0)]
    for row in range(rows):
        for column in range(columns - 1):
            strips += [(row, column, 3), (row, column + 1, 2)]
    return strips


def outer_strips(rows, columns):
    strips = [(0, column, 0) for column in range(columns)]
    strips += [(rows - 1, column, 1) for column in range(columns)]
    strips += [(row, 0, 2) for row in range(rows)]
    strips += [(row, columns - 1, 3) for row in range(rows)]
    return strips


def partner_of(strip):
    row, column, side = strip
    return [
        (row - 1, column, 1),
        (row + 1, column, 0),
        (row, column - 1, 3),
        (row, column + 1, 2),
    ][side]


def edges_kernel(w_ref, up_ref, down_ref, left_ref, right_ref):
    rows, columns = w_ref.shape[:2]
    for column in range(columns):
        up_ref[column : column + 1] = w_ref[0, column, 0:1, :]
        down_ref[column : column + 1] = w_ref[rows - 1, column, 1:2, :]
    for row in range(rows):
        left_ref[row : row + 1] = w_ref[row, 0, 2:3, :]
        right_ref[row : row + 1] = w_ref[row, columns - 1, 3:4, :]


def edges(weights):
    rows, columns, sides, length = weights.shape
    width = chunk_width(length)
    row_shape = jax.ShapeDtypeStruct((columns, length), weights.dtype)
    column_shape = jax.ShapeDtypeStruct((rows, length), weights.dtype)
    row_spec = pl.BlockSpec((columns, width), lambda i: (0, i))
    column_spec = pl.BlockSpec((rows, width), lambda i: (0, i))
    return pl.pallas_call(
        edges_kernel,
        grid=(length // width,),
        in_specs=[pl.BlockSpec((rows, columns, sides, width), lambda i: (0, 0, 0, i))],
        out_specs=[row_spec, row_spec, column_spec, column_spec],
        out_shape=[row_shape, row_shape, column_shape, column_shape],
        name="edges",
    )(weights)


def inner_kernel(dots, p_ref, w_ref, out_ref, wide, sums):
    @pl.when(pl.program_id(0) == 0)
    def _():
        sums[...] = jnp.zeros_like(sums)

    wide[...] = w_ref[...].astype(jnp.float32)

    def read_bins(strip, lanes):
        row, column, side = strip
        return p_ref[row, column, side : side + 1, lanes]

    def read_joint(strip, lanes):
        row, column, side = strip
        if side in (0, 2):
            row, column, side = partner_of(strip)
        other_row, other_column, other_side = partner_of((row, column, side))
        return (
            wide[row, column, side : side + 1, lanes]
            * wide[other_row, other_column, other_side : other_side + 1, lanes]
        )

    accumulate(dots, read_bins, read_joint, sums, p_ref.shape[-1])

    @pl.when(pl.program_id(0) == pl.num_programs(0) - 1)
    def _():
        finish(dots, sums, out_ref)


def outer_kernel(dots, p_ref, w_ref, up_ref, down_ref, left_ref, right_ref, out_ref, wide, row_wide, column_wide, sums):
    @pl.when(pl.program_id(0) == 0)
    def _():
        sums[...] = jnp.zeros_like(sums)

    wide[...] = w_ref[...].astype(jnp.float32)
    row_wide[0] = up_ref[...].astype(jnp.float32)
    row_wide[1] = down_ref[...].astype(jnp.float32)
    column_wide[0] = left_ref[...].astype(jnp.float32)
    column_wide[1] = right_ref[...].astype(jnp.float32)

    def read_bins(strip, lanes):
        row, column, side = strip
        return p_ref[row, column, side : side + 1, lanes]

    def read_joint(strip, lanes):
        row, column, side = strip
        own = wide[row, column, side : side + 1, lanes]
        if side < 2:
            return own * row_wide[side, column : column + 1, lanes]
        return own * column_wide[side - 2, row : row + 1, lanes]

    accumulate(dots, read_bins, read_joint, sums, p_ref.shape[-1])

    @pl.when(pl.program_id(0) == pl.num_programs(0) - 1)
    def _():
        finish(dots, sums, out_ref)


def strip_sums(kernel, strips, pixels, weights, halos, name):
    rows, columns, sides, length = pixels.shape
    width = chunk_width(length)
    dots = group(strips)
    block = (rows, columns, sides, width)
    halo_specs = [pl.BlockSpec((h.shape[0], width), lambda i: (0, i)) for h in halos]
    scratch = [pltpu.VMEM(block, jnp.float32)]
    if halos:
        scratch += [pltpu.VMEM((2, columns, width), jnp.float32), pltpu.VMEM((2, rows, width), jnp.float32)]
    scratch += [pltpu.VMEM((len(dots), 16 * SUBS * PER_DOT, 16 * SUBS * PER_DOT), jnp.float32)]
    return pl.pallas_call(
        functools.partial(kernel, dots),
        grid=(length // width,),
        in_specs=[pl.BlockSpec(block, lambda i: (0, 0, 0, i))] * 2 + halo_specs,
        out_specs=pl.BlockSpec((len(strips), 16, 16), lambda i: (0, 0, 0)),
        out_shape=jax.ShapeDtypeStruct((len(strips), 16, 16), jnp.float32),
        scratch_shapes=scratch,
        compiler_params=pltpu.CompilerParams(vmem_limit_bytes=56 * 1024 * 1024),
        cost_estimate=pl.CostEstimate(
            flops=len(strips) * length * 256 * 32,
            bytes_accessed=rows * columns * sides * length * 6,
            transcendentals=0,
        ),
        name=name,
    )(pixels, weights, *halos)


def shift(array, axis, step):
    count = lax.axis_size(axis)
    if step > 0:
        pairs = [(i, i + 1) for i in range(count - 1)]
    else:
        pairs = [(i + 1, i) for i in range(count - 1)]
    return lax.ppermute(array, axis, pairs)


def settle_kernel(
    inner, outer, shape, inner_ref, outer_ref, adjacency_ref, out_ref,
    row_in, column_in, own, other, tile, board, grid,
    near_send, near_recv, far_send, far_recv,
):
    rows, columns = shape
    x_count, y_count = lax.axis_size("gx"), lax.axis_size("gy")
    x_index, y_index = lax.axis_index("gx"), lax.axis_index("gy")
    devices = x_count * y_count
    me = x_index * y_count + y_index
    grid_rows, grid_columns = y_count * rows, x_count * columns
    lanes = grid.shape[1]

    def device(index):
        return {"gx": index // y_count, "gy": index % y_count}

    barrier = pltpu.get_barrier_semaphore()

    @pl.loop(1, devices)
    def _(step):
        pl.semaphore_signal(
            barrier, inc=1, device_id=device((me + step) % devices), device_id_type=pl.DeviceIdType.MESH
        )

    pl.semaphore_wait(barrier, devices - 1)

    up_copy = pltpu.make_async_remote_copy(
        src_ref=outer_ref.at[pl.ds(0, columns)], dst_ref=row_in,
        send_sem=near_send.at[0], recv_sem=near_recv.at[0],
        device_id={"gx": x_index, "gy": (y_index + y_count - 1) % y_count},
        device_id_type=pl.DeviceIdType.MESH,
    )
    left_copy = pltpu.make_async_remote_copy(
        src_ref=outer_ref.at[pl.ds(2 * columns, rows)], dst_ref=column_in,
        send_sem=near_send.at[1], recv_sem=near_recv.at[1],
        device_id={"gx": (x_index + x_count - 1) % x_count, "gy": y_index},
        device_id_type=pl.DeviceIdType.MESH,
    )
    up_copy.start()
    left_copy.start()

    where_inner = {strip: i for i, strip in enumerate(inner)}
    where_outer = {strip: i for i, strip in enumerate(outer)}

    def local(strip):
        if strip in where_inner:
            return inner_ref[where_inner[strip]]
        return outer_ref[where_outer[strip]]

    pairs = [(r, c, 1) for r in range(rows) for c in range(columns)]
    pairs += [(r, c, 3) for r in range(rows) for c in range(columns)]
    late = []
    for number, strip in enumerate(pairs):
        own[number] = local(strip)
        facing_strip = partner_of(strip)
        if facing_strip in where_inner:
            other[number] = local(facing_strip)
        else:
            late.append((number, strip))
    up_copy.wait()
    left_copy.wait()
    for number, (row, column, side) in late:
        other[number] = row_in[column] if side == 1 else column_in[row]

    count = len(pairs)
    centre = (
        16 * lax.broadcasted_iota(jnp.int32, (count, 16, 16), 1)
        + lax.broadcasted_iota(jnp.int32, (count, 16, 16), 2)
    ).astype(jnp.float32) + 0.5

    def over_bins(values):
        return jnp.sum(jnp.sum(values, axis=1, keepdims=True), axis=2, keepdims=True)

    def share_and_mean(values):
        total = over_bins(values)
        total = jnp.where(total > 0.0, total, 1.0)
        return values / total, over_bins(values * centre) / total

    own_share, own_mean = share_and_mean(own[...])
    other_share, other_mean = share_and_mean(other[...])
    gap = (own_share - other_share).reshape(count * 16, 16)
    low_a = lax.broadcasted_iota(jnp.int32, (16, 16), 0)
    low_b = lax.broadcasted_iota(jnp.int32, (16, 16), 1)
    high_a = lax.broadcasted_iota(jnp.int32, (count * 16, count * 16), 0)
    high_b = lax.broadcasted_iota(jnp.int32, (count * 16, count * 16), 1)
    within = (low_a <= low_b).astype(jnp.float32)
    before = ((high_a // 16 == high_b // 16) & (high_b < high_a)).astype(jnp.float32)
    exact = dict(precision=lax.Precision.HIGHEST, preferred_element_type=jnp.float32)
    running = jnp.dot(gap, within, **exact) + jnp.sum(
        jnp.dot(before, gap, **exact), axis=1, keepdims=True
    )
    distance = over_bins(jnp.abs(running).reshape(count, 16, 16))
    mismatch = (distance - jnp.abs(own_mean - other_mean)) / mismatch_scale
    confidence = (1.0 / (0.25 + mismatch * mismatch)).reshape(count, 1)
    offset = (jnp.log(other_mean) - jnp.log(own_mean)).reshape(count, 1)

    pair = lax.broadcasted_iota(jnp.int32, (count, lanes), 0)
    lane = lax.broadcasted_iota(jnp.int32, (count, lanes), 1)
    direction = pair // (rows * columns)
    pair_row = (pair % (rows * columns)) // columns
    spot = 2 * direction * grid_columns + x_index * columns + pair % columns
    placed = jnp.where(lane == spot, confidence, 0.0) + jnp.where(lane == spot + grid_columns, offset, 0.0)
    for row in range(rows):
        tile[row : row + 1] = jnp.sum(jnp.where(pair_row == row, placed, 0.0), axis=0, keepdims=True)
    board[x_index, y_index] = tile[...]

    def spread(index, source):
        return pltpu.make_async_remote_copy(
            src_ref=tile, dst_ref=board.at[source // y_count, source % y_count],
            send_sem=far_send.at[index], recv_sem=far_recv.at[source],
            device_id=device(index), device_id_type=pl.DeviceIdType.MESH,
        )

    @pl.loop(1, devices)
    def _(step):
        spread((me + step) % devices, me).start()

    @pl.loop(1, devices)
    def _(step):
        source = (me + step) % devices
        spread(source, source).wait_recv()

    for place in range(y_count):
        rows_here = board[0, place]
        for other_x in range(1, x_count):
            rows_here += board[other_x, place]
        grid[place * rows : (place + 1) * rows] = rows_here

    whole = grid[...]
    row_id = lax.broadcasted_iota(jnp.int32, (grid_rows, lanes), 0)
    lane_id = lax.broadcasted_iota(jnp.int32, (grid_rows, lanes), 1)

    def quantity(number, link, keep):
        values = whole if number == 0 else pltpu.roll(whole, lanes - number * grid_columns, 1)
        return jnp.where(keep, values, 0.0)

    def widened(index):
        flat = adjacency_ref[index]
        if lanes > grid_columns:
            blank = jnp.zeros((grid_rows, lanes - grid_columns), jnp.int32)
            flat = jnp.concatenate([flat, blank], axis=1)
        return flat

    keep_down = (widened(1) > 0) & (row_id < grid_rows - 1) & (lane_id < grid_columns)
    keep_right = (widened(0) > 0) & (lane_id < grid_columns - 1)
    down_conf = quantity(0, 1, keep_down)
    down_off = quantity(1, 1, keep_down)
    right_conf = quantity(2, 0, keep_right)
    right_off = quantity(3, 0, keep_right)
    up_conf, up_off = pltpu.roll(down_conf, 1, 0), -pltpu.roll(down_off, 1, 0)
    left_conf, left_off = pltpu.roll(right_conf, 1, 1), -pltpu.roll(right_off, 1, 1)
    confidence_sum = up_conf + down_conf + left_conf + right_conf
    denominator = anchor_weight + confidence_sum
    push = (
        up_conf * up_off + down_conf * down_off + left_conf * left_off + right_conf * right_off
    ) / denominator
    up_part, down_part = up_conf / denominator, down_conf / denominator
    left_part, right_part = left_conf / denominator, right_conf / denominator
    pull = confidence_sum / denominator
    tiles = grid_rows * grid_columns

    def mean_of(values):
        return jnp.sum(jnp.sum(values, axis=0, keepdims=True), axis=1, keepdims=True) / tiles

    def sweep(_, fresh):
        return (
            up_part * pltpu.roll(fresh, 1, 0)
            + down_part * pltpu.roll(fresh, grid_rows - 1, 0)
            + left_part * pltpu.roll(fresh, 1, 1)
            + right_part * pltpu.roll(fresh, lanes - 1, 1)
            + push
        ) - pull * mean_of(fresh)

    fresh = lax.fori_loop(0, ITERS - 1, sweep, push)
    log_gain = fresh - mean_of(fresh)
    result = jnp.zeros((rows, columns), jnp.float32)
    out_row = lax.broadcasted_iota(jnp.int32, (rows, columns), 0)
    out_column = lax.broadcasted_iota(jnp.int32, (rows, columns), 1)
    for row in range(rows):
        line = jnp.sum(jnp.where(row_id == y_index * rows + row, log_gain, 0.0), axis=0, keepdims=True)
        for column in range(columns):
            value = jnp.sum(
                jnp.where(lane_id[:1] == x_index * columns + column, line, 0.0), axis=1, keepdims=True
            )
            result += jnp.where((out_row == row) & (out_column == column), value, 0.0)
    out_ref[...] = result

    @pl.loop(1, devices)
    def _(step):
        spread((me + step) % devices, me).wait_send()


def settle(inner, outer, shape, inner_sums, outer_sums, adjacency):
    rows, columns = shape
    x_count, y_count = lax.axis_size("gx"), lax.axis_size("gy")
    devices = x_count * y_count
    lanes = -(-4 * x_count * columns // 128) * 128
    pairs = 2 * rows * columns
    vmem = pl.BlockSpec(memory_space=pltpu.VMEM)
    return pl.pallas_call(
        functools.partial(settle_kernel, inner, outer, shape),
        in_specs=[vmem] * 3,
        out_specs=vmem,
        out_shape=jax.ShapeDtypeStruct((rows, columns), jnp.float32),
        scratch_shapes=[
            pltpu.VMEM((columns, 16, 16), jnp.float32),
            pltpu.VMEM((rows, 16, 16), jnp.float32),
            pltpu.VMEM((pairs, 16, 16), jnp.float32),
            pltpu.VMEM((pairs, 16, 16), jnp.float32),
            pltpu.VMEM((rows, lanes), jnp.float32),
            pltpu.VMEM((x_count, y_count, rows, lanes), jnp.float32),
            pltpu.VMEM((y_count * rows, lanes), jnp.float32),
            pltpu.SemaphoreType.DMA((2,)),
            pltpu.SemaphoreType.DMA((2,)),
            pltpu.SemaphoreType.DMA((devices,)),
            pltpu.SemaphoreType.DMA((devices,)),
        ],
        compiler_params=pltpu.CompilerParams(collective_id=0, has_side_effects=True),
        name="settle",
    )(inner_sums, outer_sums, adjacency)


def body(pixels, weights, adjacency):
    rows, columns = pixels.shape[:2]
    up, down, left, right = edges(weights)
    from_up = shift(down, "gy", 1)
    from_down = shift(up, "gy", -1)
    from_left = shift(right, "gx", 1)
    from_right = shift(left, "gx", -1)
    inner = inner_strips(rows, columns)
    outer = outer_strips(rows, columns)
    inner_sums = strip_sums(inner_kernel, inner, pixels, weights, [], "inner")
    outer_sums = strip_sums(
        outer_kernel, outer, pixels, weights, [from_up, from_down, from_left, from_right], "outer"
    )
    return settle(inner, outer, (rows, columns), inner_sums, outer_sums, adjacency)


def solution(mesh):
    return jax.shard_map(
        body,
        mesh=mesh,
        in_specs=(P("gy", "gx", None, None), P("gy", "gx", None, None), P()),
        out_specs=P("gy", "gx"),
        check_vma=False,
    )
```

```python
import functools
import jax
import jax.numpy as jnp
from jax import lax
from jax.experimental import pallas as pl
from jax.experimental.pallas import tpu as pltpu
from jax.sharding import PartitionSpec as P

ITERS = 20
WIDTH = 16384
EDGE_WIDTH = 16384
SUBS = 4
PER_DOT = 4


anchor_weight = 0.5
mismatch_scale = 8.0


def chunk_width(length, width):
    while length % width:
        width //= 2
    return width


def one_hots(bins, joint, level, shape):
    bins16 = jnp.broadcast_to(bins, shape).astype(jnp.int16)
    upper = (bins16 & 240) == level * 16
    lower = (bins16 & 15) == level
    joint16 = jnp.broadcast_to(joint, shape).astype(jnp.bfloat16)
    zero = jnp.zeros(shape, jnp.bfloat16)
    return jnp.where(upper, joint16, zero), jnp.where(lower, jnp.ones(shape, jnp.bfloat16), zero)


def accumulate(dots, read_bins, read_joint, sums, width):
    depth = width // SUBS
    shape = (16, depth)
    level = lax.broadcasted_iota(jnp.int32, shape, 0).astype(jnp.int16)
    for index, strips in enumerate(dots):
        left, right = [], []
        for strip in strips:
            for sub in range(SUBS):
                lanes = slice(sub * depth, (sub + 1) * depth)
                first, second = one_hots(read_bins(strip, lanes), read_joint(strip, lanes), level, shape)
                left.append(first)
                right.append(second)
        left = jnp.concatenate(left, axis=0)
        right = jnp.concatenate(right, axis=0)
        counts = lax.dot_general(
            left, right, (((1,), (1,)), ((), ())), preferred_element_type=jnp.float32
        )
        sums[index] += counts


def finish(dots, sums, out_ref):
    place = 0
    for index, strips in enumerate(dots):
        for number in range(len(strips)):
            total = jnp.zeros((16, 16), jnp.float32)
            for sub in range(SUBS):
                start = (number * SUBS + sub) * 16
                total += sums[index, start : start + 16, start : start + 16]
            out_ref[place] = total
            place += 1


def group(strips):
    return [strips[i : i + PER_DOT] for i in range(0, len(strips), PER_DOT)]


def inner_strips(rows, columns):
    strips = []
    for row in range(rows - 1):
        for column in range(columns):
            strips += [(row, column, 1), (row + 1, column, 0)]
    for row in range(rows):
        for column in range(columns - 1):
            strips += [(row, column, 3), (row, column + 1, 2)]
    return strips


def outer_strips(rows, columns):
    strips = [(0, column, 0) for column in range(columns)]
    strips += [(rows - 1, column, 1) for column in range(columns)]
    strips += [(row, 0, 2) for row in range(rows)]
    strips += [(row, columns - 1, 3) for row in range(rows)]
    return strips


def partner_of(strip):
    row, column, side = strip
    return [
        (row - 1, column, 1),
        (row + 1, column, 0),
        (row, column - 1, 3),
        (row, column + 1, 2),
    ][side]


def edges_kernel(w_ref, up_ref, down_ref, left_ref, right_ref):
    rows, columns = w_ref.shape[:2]
    for column in range(columns):
        up_ref[column : column + 1] = w_ref[0, column, 0:1, :]
        down_ref[column : column + 1] = w_ref[rows - 1, column, 1:2, :]
    for row in range(rows):
        left_ref[row : row + 1] = w_ref[row, 0, 2:3, :]
        right_ref[row : row + 1] = w_ref[row, columns - 1, 3:4, :]


def edges(weights):
    rows, columns, sides, length = weights.shape
    width = chunk_width(length, EDGE_WIDTH)
    row_shape = jax.ShapeDtypeStruct((columns, length), weights.dtype)
    column_shape = jax.ShapeDtypeStruct((rows, length), weights.dtype)
    row_spec = pl.BlockSpec((columns, width), lambda i: (0, i))
    column_spec = pl.BlockSpec((rows, width), lambda i: (0, i))
    return pl.pallas_call(
        edges_kernel,
        grid=(length // width,),
        in_specs=[pl.BlockSpec((rows, columns, sides, width), lambda i: (0, 0, 0, i))],
        out_specs=[row_spec, row_spec, column_spec, column_spec],
        out_shape=[row_shape, row_shape, column_shape, column_shape],
        name="edges",
    )(weights)


def inner_kernel(dots, p_ref, w_ref, out_ref, wide, sums):
    @pl.when(pl.program_id(0) == 0)
    def _():
        sums[...] = jnp.zeros_like(sums)

    wide[...] = w_ref[...].astype(jnp.float32)

    def read_bins(strip, lanes):
        row, column, side = strip
        return p_ref[row, column, side : side + 1, lanes]

    def read_joint(strip, lanes):
        row, column, side = strip
        if side in (0, 2):
            row, column, side = partner_of(strip)
        other_row, other_column, other_side = partner_of((row, column, side))
        return (
            wide[row, column, side : side + 1, lanes]
            * wide[other_row, other_column, other_side : other_side + 1, lanes]
        )

    accumulate(dots, read_bins, read_joint, sums, p_ref.shape[-1])

    @pl.when(pl.program_id(0) == pl.num_programs(0) - 1)
    def _():
        finish(dots, sums, out_ref)


def outer_kernel(dots, p_ref, w_ref, up_ref, down_ref, left_ref, right_ref, out_ref, wide, row_wide, column_wide, sums):
    @pl.when(pl.program_id(0) == 0)
    def _():
        sums[...] = jnp.zeros_like(sums)

    wide[...] = w_ref[...].astype(jnp.float32)
    row_wide[0] = up_ref[...].astype(jnp.float32)
    row_wide[1] = down_ref[...].astype(jnp.float32)
    column_wide[0] = left_ref[...].astype(jnp.float32)
    column_wide[1] = right_ref[...].astype(jnp.float32)

    def read_bins(strip, lanes):
        row, column, side = strip
        return p_ref[row, column, side : side + 1, lanes]

    def read_joint(strip, lanes):
        row, column, side = strip
        own = wide[row, column, side : side + 1, lanes]
        if side < 2:
            return own * row_wide[side, column : column + 1, lanes]
        return own * column_wide[side - 2, row : row + 1, lanes]

    accumulate(dots, read_bins, read_joint, sums, p_ref.shape[-1])

    @pl.when(pl.program_id(0) == pl.num_programs(0) - 1)
    def _():
        finish(dots, sums, out_ref)


def strip_sums(kernel, strips, pixels, weights, halos, name):
    rows, columns, sides, length = pixels.shape
    width = chunk_width(length, WIDTH)
    dots = group(strips)
    block = (rows, columns, sides, width)
    halo_specs = [pl.BlockSpec((h.shape[0], width), lambda i: (0, i)) for h in halos]
    scratch = [pltpu.VMEM(block, jnp.float32)]
    if halos:
        scratch += [pltpu.VMEM((2, columns, width), jnp.float32), pltpu.VMEM((2, rows, width), jnp.float32)]
    scratch += [pltpu.VMEM((len(dots), 16 * SUBS * PER_DOT, 16 * SUBS * PER_DOT), jnp.float32)]
    return pl.pallas_call(
        functools.partial(kernel, dots),
        grid=(length // width,),
        in_specs=[pl.BlockSpec(block, lambda i: (0, 0, 0, i))] * 2 + halo_specs,
        out_specs=pl.BlockSpec((len(strips), 16, 16), lambda i: (0, 0, 0)),
        out_shape=jax.ShapeDtypeStruct((len(strips), 16, 16), jnp.float32),
        scratch_shapes=scratch,
        compiler_params=pltpu.CompilerParams(vmem_limit_bytes=56 * 1024 * 1024),
        cost_estimate=pl.CostEstimate(
            flops=len(strips) * length * 256 * 32,
            bytes_accessed=rows * columns * sides * length * 6,
            transcendentals=0,
        ),
        name=name,
    )(pixels, weights, *halos)


def shift(array, axis, step):
    count = lax.axis_size(axis)
    if step > 0:
        pairs = [(i, i + 1) for i in range(count - 1)]
    else:
        pairs = [(i + 1, i) for i in range(count - 1)]
    return lax.ppermute(array, axis, pairs)


def settle_kernel(
    inner, outer, shape, inner_ref, outer_ref, adjacency_ref, out_ref,
    row_in, column_in, own, other, tile, board, grid,
    near_send, near_recv, far_send, far_recv,
):
    rows, columns = shape
    x_count, y_count = lax.axis_size("gx"), lax.axis_size("gy")
    x_index, y_index = lax.axis_index("gx"), lax.axis_index("gy")
    devices = x_count * y_count
    me = x_index * y_count + y_index
    grid_rows, grid_columns = y_count * rows, x_count * columns
    lanes = grid.shape[1]

    def device(index):
        return {"gx": index // y_count, "gy": index % y_count}

    barrier = pltpu.get_barrier_semaphore()

    @pl.loop(1, devices)
    def _(step):
        pl.semaphore_signal(
            barrier, inc=1, device_id=device((me + step) % devices), device_id_type=pl.DeviceIdType.MESH
        )

    pl.semaphore_wait(barrier, devices - 1)

    up_copy = pltpu.make_async_remote_copy(
        src_ref=outer_ref.at[pl.ds(0, columns)], dst_ref=row_in,
        send_sem=near_send.at[0], recv_sem=near_recv.at[0],
        device_id={"gx": x_index, "gy": (y_index + y_count - 1) % y_count},
        device_id_type=pl.DeviceIdType.MESH,
    )
    left_copy = pltpu.make_async_remote_copy(
        src_ref=outer_ref.at[pl.ds(2 * columns, rows)], dst_ref=column_in,
        send_sem=near_send.at[1], recv_sem=near_recv.at[1],
        device_id={"gx": (x_index + x_count - 1) % x_count, "gy": y_index},
        device_id_type=pl.DeviceIdType.MESH,
    )
    up_copy.start()
    left_copy.start()

    where_inner = {strip: i for i, strip in enumerate(inner)}
    where_outer = {strip: i for i, strip in enumerate(outer)}

    def local(strip):
        if strip in where_inner:
            return inner_ref[where_inner[strip]]
        return outer_ref[where_outer[strip]]

    pairs = [(r, c, 1) for r in range(rows) for c in range(columns)]
    pairs += [(r, c, 3) for r in range(rows) for c in range(columns)]
    late = []
    for number, strip in enumerate(pairs):
        own[number] = local(strip)
        facing_strip = partner_of(strip)
        if facing_strip in where_inner:
            other[number] = local(facing_strip)
        else:
            late.append((number, strip))
    up_copy.wait()
    left_copy.wait()
    for number, (row, column, side) in late:
        other[number] = row_in[column] if side == 1 else column_in[row]

    count = len(pairs)
    centre = (
        16 * lax.broadcasted_iota(jnp.int32, (count, 16, 16), 1)
        + lax.broadcasted_iota(jnp.int32, (count, 16, 16), 2)
    ).astype(jnp.float32) + 0.5

    def over_bins(values):
        return jnp.sum(jnp.sum(values, axis=1, keepdims=True), axis=2, keepdims=True)

    def share_and_mean(values):
        total = over_bins(values)
        total = jnp.where(total > 0.0, total, 1.0)
        return values / total, over_bins(values * centre) / total

    own_share, own_mean = share_and_mean(own[...])
    other_share, other_mean = share_and_mean(other[...])
    gap = (own_share - other_share).reshape(count * 16, 16)
    low_a = lax.broadcasted_iota(jnp.int32, (16, 16), 0)
    low_b = lax.broadcasted_iota(jnp.int32, (16, 16), 1)
    high_a = lax.broadcasted_iota(jnp.int32, (count * 16, count * 16), 0)
    high_b = lax.broadcasted_iota(jnp.int32, (count * 16, count * 16), 1)
    within = (low_a <= low_b).astype(jnp.float32)
    before = ((high_a // 16 == high_b // 16) & (high_b < high_a)).astype(jnp.float32)
    exact = dict(precision=lax.Precision.HIGHEST, preferred_element_type=jnp.float32)
    running = jnp.dot(gap, within, **exact) + jnp.sum(
        jnp.dot(before, gap, **exact), axis=1, keepdims=True
    )
    distance = over_bins(jnp.abs(running).reshape(count, 16, 16))
    mismatch = (distance - jnp.abs(own_mean - other_mean)) / mismatch_scale
    confidence = (1.0 / (0.25 + mismatch * mismatch)).reshape(count, 1)
    offset = (jnp.log(other_mean) - jnp.log(own_mean)).reshape(count, 1)

    pair = lax.broadcasted_iota(jnp.int32, (count, lanes), 0)
    lane = lax.broadcasted_iota(jnp.int32, (count, lanes), 1)
    direction = pair // (rows * columns)
    pair_row = (pair % (rows * columns)) // columns
    spot = 2 * direction * grid_columns + x_index * columns + pair % columns
    placed = jnp.where(lane == spot, confidence, 0.0) + jnp.where(lane == spot + grid_columns, offset, 0.0)
    for row in range(rows):
        tile[row : row + 1] = jnp.sum(jnp.where(pair_row == row, placed, 0.0), axis=0, keepdims=True)
    board[x_index, y_index] = tile[...]

    def spread(index, source):
        return pltpu.make_async_remote_copy(
            src_ref=tile, dst_ref=board.at[source // y_count, source % y_count],
            send_sem=far_send.at[index], recv_sem=far_recv.at[source],
            device_id=device(index), device_id_type=pl.DeviceIdType.MESH,
        )

    @pl.loop(1, devices)
    def _(step):
        spread((me + step) % devices, me).start()

    @pl.loop(1, devices)
    def _(step):
        source = (me + step) % devices
        spread(source, source).wait_recv()

    for place in range(y_count):
        rows_here = board[0, place]
        for other_x in range(1, x_count):
            rows_here += board[other_x, place]
        grid[place * rows : (place + 1) * rows] = rows_here

    whole = grid[...]
    row_id = lax.broadcasted_iota(jnp.int32, (grid_rows, lanes), 0)
    lane_id = lax.broadcasted_iota(jnp.int32, (grid_rows, lanes), 1)

    def quantity(number, link, keep):
        values = whole if number == 0 else pltpu.roll(whole, lanes - number * grid_columns, 1)
        return jnp.where(keep, values, 0.0)

    def widened(index):
        flat = adjacency_ref[index]
        if lanes > grid_columns:
            blank = jnp.zeros((grid_rows, lanes - grid_columns), jnp.int32)
            flat = jnp.concatenate([flat, blank], axis=1)
        return flat

    keep_down = (widened(1) > 0) & (row_id < grid_rows - 1) & (lane_id < grid_columns)
    keep_right = (widened(0) > 0) & (lane_id < grid_columns - 1)
    down_conf = quantity(0, 1, keep_down)
    down_off = quantity(1, 1, keep_down)
    right_conf = quantity(2, 0, keep_right)
    right_off = quantity(3, 0, keep_right)
    up_conf, up_off = pltpu.roll(down_conf, 1, 0), -pltpu.roll(down_off, 1, 0)
    left_conf, left_off = pltpu.roll(right_conf, 1, 1), -pltpu.roll(right_off, 1, 1)
    confidence_sum = up_conf + down_conf + left_conf + right_conf
    denominator = anchor_weight + confidence_sum
    push = (
        up_conf * up_off + down_conf * down_off + left_conf * left_off + right_conf * right_off
    ) / denominator
    up_part, down_part = up_conf / denominator, down_conf / denominator
    left_part, right_part = left_conf / denominator, right_conf / denominator
    pull = confidence_sum / denominator
    tiles = grid_rows * grid_columns

    def mean_of(values):
        return jnp.sum(jnp.sum(values, axis=0, keepdims=True), axis=1, keepdims=True) / tiles

    def sweep(_, fresh):
        return (
            up_part * pltpu.roll(fresh, 1, 0)
            + down_part * pltpu.roll(fresh, grid_rows - 1, 0)
            + left_part * pltpu.roll(fresh, 1, 1)
            + right_part * pltpu.roll(fresh, lanes - 1, 1)
            + push
        ) - pull * mean_of(fresh)

    fresh = lax.fori_loop(0, ITERS - 1, sweep, push)
    log_gain = fresh - mean_of(fresh)
    result = jnp.zeros((rows, columns), jnp.float32)
    out_row = lax.broadcasted_iota(jnp.int32, (rows, columns), 0)
    out_column = lax.broadcasted_iota(jnp.int32, (rows, columns), 1)
    for row in range(rows):
        line = jnp.sum(jnp.where(row_id == y_index * rows + row, log_gain, 0.0), axis=0, keepdims=True)
        for column in range(columns):
            value = jnp.sum(
                jnp.where(lane_id[:1] == x_index * columns + column, line, 0.0), axis=1, keepdims=True
            )
            result += jnp.where((out_row == row) & (out_column == column), value, 0.0)
    out_ref[...] = result

    @pl.loop(1, devices)
    def _(step):
        spread((me + step) % devices, me).wait_send()


def settle(inner, outer, shape, inner_sums, outer_sums, adjacency):
    rows, columns = shape
    x_count, y_count = lax.axis_size("gx"), lax.axis_size("gy")
    devices = x_count * y_count
    lanes = -(-4 * x_count * columns // 128) * 128
    pairs = 2 * rows * columns
    vmem = pl.BlockSpec(memory_space=pltpu.VMEM)
    return pl.pallas_call(
        functools.partial(settle_kernel, inner, outer, shape),
        in_specs=[vmem] * 3,
        out_specs=vmem,
        out_shape=jax.ShapeDtypeStruct((rows, columns), jnp.float32),
        scratch_shapes=[
            pltpu.VMEM((columns, 16, 16), jnp.float32),
            pltpu.VMEM((rows, 16, 16), jnp.float32),
            pltpu.VMEM((pairs, 16, 16), jnp.float32),
            pltpu.VMEM((pairs, 16, 16), jnp.float32),
            pltpu.VMEM((rows, lanes), jnp.float32),
            pltpu.VMEM((x_count, y_count, rows, lanes), jnp.float32),
            pltpu.VMEM((y_count * rows, lanes), jnp.float32),
            pltpu.SemaphoreType.DMA((2,)),
            pltpu.SemaphoreType.DMA((2,)),
            pltpu.SemaphoreType.DMA((devices,)),
            pltpu.SemaphoreType.DMA((devices,)),
        ],
        compiler_params=pltpu.CompilerParams(collective_id=0, has_side_effects=True),
        name="settle",
    )(inner_sums, outer_sums, adjacency)


def body(pixels, weights, adjacency):
    rows, columns = pixels.shape[:2]
    up, down, left, right = edges(weights)
    from_up = shift(down, "gy", 1)
    from_down = shift(up, "gy", -1)
    from_left = shift(right, "gx", 1)
    from_right = shift(left, "gx", -1)
    inner = inner_strips(rows, columns)
    outer = outer_strips(rows, columns)
    inner_sums = strip_sums(inner_kernel, inner, pixels, weights, [], "inner")
    outer_sums = strip_sums(
        outer_kernel, outer, pixels, weights, [from_up, from_down, from_left, from_right], "outer"
    )
    return settle(inner, outer, (rows, columns), inner_sums, outer_sums, adjacency)


def solution(mesh):
    return jax.shard_map(
        body,
        mesh=mesh,
        in_specs=(P("gy", "gx", None, None), P("gy", "gx", None, None), P()),
        out_specs=P("gy", "gx"),
        check_vma=False,
    )
```
